32 devices in a mesh: sys: 1 (over z), seg: 32 (over y, x, core).
Axes of the slice: x: 4, y: 4, z: 1, core: 2. Of those that a mesh axis runs over, the one named last changes fastest.
The devices are a block of a 4x4x8 slice.
Arguments:
- positions: bfloat16 [65536, 768], P(('sys', 'seg'))
- charges: float32 [65536], P(('sys', 'seg'))
- pair_band: int32 [32, 25], P(('sys', 'seg'))
Outputs:
- output 1: float32 [65536, 768], P(('sys', 'seg'))
- output 2: float32 [1], P('sys')
All inputs are finite; a program needn't handle non-finite values.
Results may differ from the reference program's by a relative error of at most 0.0015.
Values are sent between devices in bfloat16 or wider.
A program may use at most 768 MiB of HBM per device.

```python
import jax
import jax.numpy as jnp
from jax import lax

SEG_COUNT = 32
BLOCK_ROWS = 2048
FEAT_DIM = 768
REACH_STEPS = 12


def draw_band(mask_key):
    coin_draw = jax.random.randint(mask_key, (SEG_COUNT, REACH_STEPS), 0, 3)
    block_ids = jnp.arange(SEG_COUNT)[:, None]
    step_ids = jnp.arange(REACH_STEPS)[None, :]
    upper_cols = jnp.where((block_ids == 0) & (step_ids == REACH_STEPS - 1), 1, (coin_draw > 0).astype(jnp.int32))
    lower_list = [jnp.roll(upper_cols[:, step_idx - 1], step_idx) for step_idx in range(REACH_STEPS, 0, -1)]
    higher_list = [upper_cols[:, step_idx - 1] for step_idx in range(1, REACH_STEPS + 1)]
    centre_list = [jnp.ones((SEG_COUNT,), jnp.int32)]
    return jnp.stack(lower_list + centre_list + higher_list, axis=1).astype(jnp.int32)


def setup_inputs(seed: int = 0, part: int = 0) -> dict:
    part_key = jax.random.fold_in(jax.random.key(seed), part)
    pos_key, sign_key, mag_key, mask_key = jax.random.split(part_key, 4)
    all_rows = SEG_COUNT * BLOCK_ROWS
    pos_vals = jax.random.normal(pos_key, (all_rows, FEAT_DIM), jnp.float32)
    sign_vals = 2.0 * jax.random.randint(sign_key, (all_rows,), 0, 2).astype(jnp.float32) - 1.0
    magnitude = jax.random.uniform(mag_key, (all_rows,), jnp.float32, 0.5, 1.5)
    charge_scale = FEAT_DIM ** 0.5 * (BLOCK_ROWS * (2 * REACH_STEPS + 1)) ** -0.25
    return {'positions': pos_vals.astype(jnp.bfloat16), 'charges': sign_vals * magnitude * charge_scale, 'pair_band': draw_band(mask_key)}


def reference(positions, charges, pair_band):
    inv_lsq = 1.0 / FEAT_DIM
    pos_blocks = positions.reshape(SEG_COUNT, BLOCK_ROWS, FEAT_DIM)
    charge_blocks = charges.reshape(SEG_COUNT, BLOCK_ROWS)
    row_ids = jnp.arange(BLOCK_ROWS)
    self_pair = row_ids[:, None] == row_ids[None, :]
    offsets = jnp.arange(-REACH_STEPS, REACH_STEPS + 1)

    def one_block(host_blk):
        x_host = pos_blocks[host_blk]
        host_f32 = x_host.astype(jnp.float32)
        host_sq = jnp.sum(host_f32 * host_f32, axis=1)
        q_host = charge_blocks[host_blk]

        def one_offset(carry_state, offset):
            force_acc, energy_acc = carry_state
            other_blk = (host_blk + offset) % SEG_COUNT
            x_other = pos_blocks[other_blk]
            other_f32 = x_other.astype(jnp.float32)
            other_sq = jnp.sum(other_f32 * other_f32, axis=1)
            cross_dot = jnp.dot(x_host, x_other.T, preferred_element_type=jnp.float32)
            sq_dist = jnp.maximum(host_sq[:, None] + other_sq[None, :] - 2.0 * cross_dot, 0.0)
            weights = q_host[:, None] * charge_blocks[other_blk][None, :] * jnp.exp(sq_dist * (-0.5 * inv_lsq))
            keep_pair = (pair_band[host_blk, REACH_STEPS + offset] != 0) & jnp.logical_not(self_pair & (offset == 0))
            weights = jnp.where(keep_pair, weights, 0.0)
            pull_term = jnp.dot(weights.astype(jnp.bfloat16), x_other, preferred_element_type=jnp.float32)
            force_acc = force_acc + (jnp.sum(weights, axis=1)[:, None] * host_f32 - pull_term) * inv_lsq
            energy_acc = energy_acc + 0.5 * jnp.sum(weights)
            return (force_acc, energy_acc), None

        init_carry = (jnp.zeros((BLOCK_ROWS, FEAT_DIM), jnp.float32), jnp.zeros((), jnp.float32))
        (force_blk, energy_blk), _ = lax.scan(one_offset, init_carry, offsets)
        return force_blk, energy_blk

    force_blocks, block_energy = lax.map(one_block, jnp.arange(SEG_COUNT))
    return force_blocks.reshape(SEG_COUNT * BLOCK_ROWS, FEAT_DIM), jnp.sum(block_energy).reshape(1)
```

```python
import functools
import math

import jax
import jax.numpy as jnp
from jax import lax
from jax.experimental import pallas as pl
from jax.experimental.pallas import tpu as pltpu
from jax.sharding import PartitionSpec as P


TILE_ROWS = 512
TILE_COLS = 1024
PIECES = 2
QUOTAS = (5, 10, 10, 7, 4)
AUX_ROWS = 16
EDGE = 99
LOG2E = math.log2(math.e)


def split3(v):
    hi = v.astype(jnp.bfloat16).astype(jnp.float32)
    rest = v - hi
    mid = rest.astype(jnp.bfloat16).astype(jnp.float32)
    return hi, mid, rest - mid


def pack_call(x_rows, charges):
    n_rows, feat = x_rows.shape
    piece = n_rows // PIECES
    step = 128

    def kernel(x_ref, q_ref, *outs):
        packs, (shift_ref, charge_ref) = outs[:PIECES], outs[PIECES:]
        for h in range(PIECES):
            shift_row, charge_row = [], []
            for b in range(piece // step):
                row0 = h * piece + b * step
                x32 = x_ref[row0:row0 + step, :].astype(jnp.float32)
                shift = jnp.sum(x32 * x32, axis=1, keepdims=True) * (-0.5 / feat * LOG2E)
                shift = jnp.broadcast_to(shift, (step, step))
                shift_ref[row0:row0 + step, :] = shift
                q_row = q_ref[row0 // step:row0 // step + 1, :]
                charge_ref[row0:row0 + step, :] = jnp.broadcast_to(q_row, (step, step)).T
                shift_row.append(shift.T[:1, :])
                charge_row.append(q_row)
            packs[h][:piece, :] = x_ref[h * piece:(h + 1) * piece, :]
            aux = []
            for row in (jnp.concatenate(shift_row, axis=1), jnp.concatenate(charge_row, axis=1)):
                for part in split3(row):
                    aux.append(part[:, :feat])
                    aux.append(jnp.concatenate([part[:, feat:], jnp.zeros((1, 2 * feat - piece), jnp.float32)], axis=1))
            aux.append(jnp.zeros((AUX_ROWS - len(aux), feat), jnp.float32))
            packs[h][piece:, :] = jnp.concatenate(aux, axis=0).astype(jnp.bfloat16)

    vmem = pl.BlockSpec(memory_space=pltpu.VMEM)
    spread = jax.ShapeDtypeStruct((n_rows, step), jnp.float32)
    return pl.pallas_call(
        kernel,
        out_shape=[jax.ShapeDtypeStruct((piece + AUX_ROWS, feat), jnp.bfloat16)] * PIECES + [spread, spread],
        in_specs=[vmem, vmem],
        out_specs=[vmem] * (PIECES + 2),
        name="pack_rows",
    )(x_rows, charges.reshape(n_rows // step, step))


def pair_call(sites, cols, done, quota, band, x_rows, row_shift, row_charge, carry, site_block, final=False):
    n_rows, feat = x_rows.shape
    piece = cols[0].shape[0] - AUX_ROWS
    n_bufs = len(cols)
    inv_lsq = 1.0 / feat
    dot_scale = inv_lsq * LOG2E
    tr, tc = TILE_ROWS, TILE_COLS
    n_chunk = piece // tc
    n_bands = n_rows // tr
    n_tiles = n_bands * n_chunk
    first = carry is None

    def kernel(*refs):
        band_ref, shift_ref, charge_ref, x_hbm = refs[:4]
        refs = refs[4:]
        col_refs, refs = refs[:n_bufs], refs[n_bufs:]
        if not first:
            (p_in, r_in, next_in), refs = refs[:3], refs[3:]
        (p_out, r_out, next_out), refs = refs[:3], refs[3:]
        x_v, p_v, r_v, col_v, aux_v, dot_v, list_ref, sems, x_sems, p_sems, r_sem = refs

        n_live = jnp.int32(0)
        start = jnp.int32(0) if first else next_in[0]
        nxt = start
        for k, site in enumerate(sites):
            col, ok = site_block(site)
            take = ok & (band_ref[0, col] != 0) & (start <= done + k) & (n_live < quota)
            list_ref[n_live] = k
            n_live = n_live + take.astype(jnp.int32)
            nxt = jnp.where((start <= done + k) & ((n_live < quota) | take), done + k + 1, nxt)
        next_out[0] = nxt
        n_all = n_live * n_tiles

        def col_start(item):
            slot = list_ref[item]
            par = lax.rem(item, 2)
            for k in range(n_bufs):
                @pl.when(slot == k)
                def _(k=k):
                    pltpu.make_async_copy(col_refs[k], col_v.at[par], sems.at[par]).start()

        def col_wait(item):
            par = lax.rem(item, 2)
            pltpu.make_async_copy(col_refs[0], col_v.at[par], sems.at[par]).wait()
            aux = col_v[par, piece:, :].astype(jnp.float32)
            for v in range(2):
                r = 6 * v
                wide = aux[r:r + 1, :] + aux[r + 2:r + 3, :] + aux[r + 4:r + 5, :]
                tail = aux[r + 1:r + 2, :] + aux[r + 3:r + 4, :] + aux[r + 5:r + 6, :]
                aux_v[par, v, :, :feat] = wide
                aux_v[par, v, :, feat:] = tail[:, :piece - feat]

        def place(t):
            item = t // n_tiles
            local = lax.rem(t, n_tiles)
            row0 = pl.multiple_of((local // n_chunk) * tr, tr)
            col0 = pl.multiple_of(lax.rem(local, n_chunk) * tc, tc)
            return item, row0, col0

        def dots(t, dst):
            item, row0, col0 = place(jnp.minimum(t, n_all - 1))
            dot_v[dst] = lax.dot_general(
                x_v[pl.ds(row0, tr), :], col_v[lax.rem(item, 2), pl.ds(col0, tc), :],
                (((1,), (1,)), ((), ())), preferred_element_type=jnp.float32)

        def pulls(t, src):
            item, row0, col0 = place(t)
            par = lax.rem(item, 2)
            shift_r = shift_ref[pl.ds(row0, tr), :]
            charge_r = charge_ref[pl.ds(row0, tr), :]
            if first:
                gap = lax.broadcasted_iota(jnp.int32, (tr, 128), 1) - lax.broadcasted_iota(jnp.int32, (tr, 128), 0)
                diag = row0 - list_ref[item] * piece - col0
            row_sum = None
            low = []
            for j in range(tc // 128):
                at = pl.multiple_of(col0 + j * 128, 128)
                shift_c = aux_v[par, 0, :, pl.ds(at, 128)]
                charge_c = aux_v[par, 1, :, pl.ds(at, 128)]
                expo = jnp.minimum(dot_v[src, :, j * 128:(j + 1) * 128] * dot_scale + (shift_r + shift_c), 0.0)
                w = jnp.exp2(expo) * (charge_r * charge_c)
                if first:
                    w = jnp.where(gap + j * 128 == diag, 0.0, w)
                row_sum = w if row_sum is None else row_sum + w
                low.append(w.astype(jnp.bfloat16))
            r_v[pl.ds(row0, tr), :] += row_sum
            p_v[pl.ds(row0, tr), :] += jnp.dot(
                jnp.concatenate(low, axis=1), col_v[par, pl.ds(col0, tc), :], preferred_element_type=jnp.float32)

        def rows_of(i):
            return pl.ds(pl.multiple_of(i * tr, tr), tr)

        def x_load(i):
            return pltpu.make_async_copy(x_hbm.at[rows_of(i)], x_v.at[rows_of(i)], x_sems.at[i])

        def p_load(i):
            return pltpu.make_async_copy(p_in.at[rows_of(i)], p_v.at[rows_of(i)], p_sems.at[i])

        def p_store(i):
            return pltpu.make_async_copy(p_v.at[rows_of(i)], p_out.at[rows_of(i)], p_sems.at[i])

        def band_of(t):
            return lax.rem(t, n_tiles) // n_chunk

        def begin():
            x_load(0).start()
            for i in range(1, n_bands):
                x_load(i).start()
            if first:
                p_v[...] = jnp.zeros_like(p_v)
                r_v[...] = jnp.zeros_like(r_v)
            else:
                pltpu.make_async_copy(r_in, r_v, r_sem).start()
                for i in range(n_bands):
                    p_load(i).start()

        def sums():
            col_wait(0)
            x_load(0).wait()
            dots(0, 0)
            for i in range(1, n_bands):
                x_load(i).wait()
            if not first:
                pltpu.make_async_copy(r_in, r_v, r_sem).wait()

            @pl.loop(0, n_all // 2)
            def _(u):
                t = u * 2
                item = t // n_tiles
                local = lax.rem(t, n_tiles)

                @pl.when((local == 0) & (item + 1 < n_live))
                def _():
                    col_start(item + 1)

                @pl.when((local + 2 == n_tiles) & (item + 1 < n_live))
                def _():
                    col_wait(item + 1)

                if not first:
                    @pl.when(item == 0)
                    def _():
                        p_load(local).wait()
                        p_load(local + 1).wait()

                dots(t + 1, 1)
                pulls(t, 0)
                dots(t + 2, 0)
                pulls(t + 1, 1)

                if not final:
                    @pl.when(item + 1 == n_live)
                    def _():
                        p_store(local).start()
                        p_store(local + 1).start()

            if not final:
                r_store = pltpu.make_async_copy(r_v, r_out, r_sem)
                r_store.start()
                for i in range(n_bands):
                    p_store(i).wait()
                r_store.wait()

        if not final:
            @pl.when(n_live > 0)
            def _():
                col_start(0)
                begin()
                sums()
        else:
            @pl.when(n_live > 0)
            def _():
                col_start(0)
            begin()

            @pl.when(n_live > 0)
            def _():
                sums()

            @pl.when(n_live == 0)
            def _():
                for i in range(n_bands):
                    x_load(i).wait()
                    p_load(i).wait()
                pltpu.make_async_copy(r_in, r_v, r_sem).wait()

            share = jnp.zeros((8, 128), jnp.float32)
            for i in range(n_bands):
                for h in range(tr // 128):
                    rows = slice(i * tr + h * 128, i * tr + (h + 1) * 128)
                    lanes = r_v[rows, :]
                    for g in range(16):
                        share = share + lanes[g * 8:(g + 1) * 8, :]
                    total = jnp.sum(lanes, axis=1, keepdims=True)
                    p_v[rows, :] = (total * x_v[rows, :].astype(jnp.float32) - p_v[rows, :]) * inv_lsq
                p_store(i).start()
            r_v[:8, :] = share
            share_out = pltpu.make_async_copy(r_v.at[:8], r_out, r_sem)
            share_out.start()
            for i in range(n_bands):
                p_store(i).wait()
            share_out.wait()

    assert n_chunk == 1 and n_tiles % 2 == 0
    smem = pl.BlockSpec(memory_space=pltpu.SMEM)
    vmem = pl.BlockSpec(memory_space=pltpu.VMEM)
    hbm = pl.BlockSpec(memory_space=pl.ANY)
    args = [band, row_shift, row_charge, x_rows] + list(cols)
    specs = [smem, vmem, vmem, hbm] + [hbm] * n_bufs
    aliases = {}
    if not first:
        aliases = {len(args): 0} if final else {len(args): 0, len(args) + 1: 1}
        args += list(carry)
        specs += [hbm, hbm, smem]
    flops = int(4 * n_rows * piece * feat * min(quota, 2 * n_bufs // 3 + 1))
    return pl.pallas_call(
        kernel,
        out_shape=(jax.ShapeDtypeStruct((n_rows, feat), jnp.float32),
                   jax.ShapeDtypeStruct((8 if final else n_rows, 128), jnp.float32),
                   jax.ShapeDtypeStruct((1,), jnp.int32)),
        in_specs=specs,
        out_specs=(hbm, hbm, smem),
        input_output_aliases=aliases,
        scratch_shapes=[
            pltpu.VMEM((n_rows, feat), jnp.bfloat16),
            pltpu.VMEM((n_rows, feat), jnp.float32),
            pltpu.VMEM((n_rows, 128), jnp.float32),
            pltpu.VMEM((2, piece + AUX_ROWS, feat), jnp.bfloat16),
            pltpu.VMEM((2, 2, 1, piece), jnp.float32),
            pltpu.VMEM((2, tr, tc), jnp.float32),
            pltpu.SMEM((n_bufs + 1,), jnp.int32),
            pltpu.SemaphoreType.DMA((2,)),
            pltpu.SemaphoreType.DMA((n_bands,)),
            pltpu.SemaphoreType.DMA((n_bands,)),
            pltpu.SemaphoreType.DMA,
        ],
        cost_estimate=pl.CostEstimate(flops=flops, bytes_accessed=4 * n_rows * feat * 4, transcendentals=0),
        compiler_params=pltpu.CompilerParams(vmem_limit_bytes=60000 * 1024),
        name="pair_pulls",
    )(*args)


def energy_call(part, seg_len):
    def kernel(part_ref, out_ref, held, send_sems, recv_sems):
        me = lax.axis_index('seg')
        barrier = pltpu.get_barrier_semaphore()
        for k in range(1, seg_len):
            pl.semaphore_signal(barrier, inc=1, device_id={'seg': lax.rem(me + k, seg_len)})
        pl.semaphore_wait(barrier, seg_len - 1)
        copies = [pltpu.make_async_remote_copy(
            src_ref=part_ref, dst_ref=held.at[me], send_sem=send_sems.at[k], recv_sem=recv_sems.at[k],
            device_id={'seg': lax.rem(me + k, seg_len)}) for k in range(1, seg_len)]
        for c in copies:
            c.start()
        held[me] = part_ref[...]
        for c in copies:
            c.wait()
        total = held[0]
        for k in range(1, seg_len):
            total = total + held[k]
        out_ref[...] = total

    vmem = pl.BlockSpec(memory_space=pltpu.VMEM)
    return pl.pallas_call(
        kernel,
        out_shape=jax.ShapeDtypeStruct(part.shape, jnp.float32),
        in_specs=[vmem],
        out_specs=vmem,
        scratch_shapes=[pltpu.VMEM((seg_len,) + part.shape, jnp.float32),
                        pltpu.SemaphoreType.DMA((seg_len,)), pltpu.SemaphoreType.DMA((seg_len,))],
        compiler_params=pltpu.CompilerParams(collective_id=0, has_side_effects=True),
        name="energy_sum",
    )(part)


def solution(mesh):
    seg_len = mesh.shape['seg']
    side = math.isqrt(seg_len // 2)

    def dev(x, y, core):
        return ((y % side) * side + x % side) * 2 + core

    grid = [(x, y, core) for y in range(side) for x in range(side) for core in range(2)]

    def come_from(values, dx, dy):
        return lax.ppermute(values, 'seg', [(dev(x + dx, y + dy, c), dev(x, y, c)) for x, y, c in grid])

    def other_core(value):
        return lax.ppermute(value, 'seg', [(dev(x, y, 1 - c), dev(x, y, c)) for x, y, c in grid])

    def device_fn(positions, charges, pair_band):
        reach = (pair_band.shape[1] - 1) // 2

        def site_block(site):
            dx, dy, flip = site
            me = lax.axis_index('seg')
            core, chip = lax.rem(me, 2), me // 2
            x, y = lax.rem(chip, side), chip // side
            if dx == EDGE:
                dx = jnp.where(x == 0, side - 1, jnp.where(x == side - 1, 1, 0))
            else:
                dx = dx % side
            blk = (lax.rem(y + dy % side, side) * side + lax.rem(x + dx, side)) * 2 + lax.rem(core + flip, 2)
            gap = lax.rem(blk - me + seg_len + seg_len // 2, seg_len) - seg_len // 2
            ok = (gap <= reach) & (gap >= -reach)
            if site[0] == EDGE:
                ok = ok & ((x == 0) | (x == side - 1))
            return jnp.where(ok, gap + reach, 0), ok

        pack_and_rows = pack_call(positions, charges)
        own, (row_shift, row_charge) = pack_and_rows[:PIECES], pack_and_rows[PIECES:]
        band = pair_band
        axis_y = lax.axis_index('seg') // 2
        my_x = lax.rem(axis_y, side)

        near = ((1, 0), (-1, 0), (0, 1), (0, -1))
        second = {(2, 0): ((1, 0), (1, 0)), (-1, -1): ((0, -1), (-1, 0)), (1, 1): ((1, 0), (0, 1)), (1, -1): ((1, 0), (0, -1))}
        third = {(-1, 1): ((0, 1), (-1, 0)), (2, 1): ((2, 0), (0, 1)), (2, -1): ((2, 0), (0, -1))}
        edge_perm = [(dev(0, y + 1, c), dev(0, y, c)) for y in range(side) for c in range(2)]
        edge_perm += [(dev(side - 1, y - 1, c), dev(side - 1, y, c)) for y in range(side) for c in range(2)]

        def hop(held, table):
            return {off: come_from(held[src], *step) for off, (src, step) in table.items()}

        def last_hop(held, h):
            src, step = (((2, 1), (0, 1)), ((2, -1), (0, -1)))[h % 2]
            edge = jnp.where(my_x == 0, held[(-1, 1)], held[(1, -1)])
            return {(2, 2): come_from(held[src], *step), (EDGE, 2): lax.ppermute(edge, 'seg', edge_perm)}

        def swap(held, offs):
            return {off: other_core(held[off]) for off in offs}

        queue = []
        lowest = [0]

        def arrive(held, flip):
            for off, value in held.items():
                queue.append((off + (flip,), value))

        def sum_some(carry, quota, final=False):
            low = lowest[0]
            sites, cols = zip(*queue[low:])
            lowest[0] = min(len(queue), low + quota)
            return pair_call(sites, cols, low, quota, band, positions, row_shift, row_charge, carry, site_block, final)

        gate = lax.optimization_barrier
        twin = [{(0, 0): other_core(o)} for o in own]
        a, b = [{off: come_from(o, *off) for off in near} for o in own]
        carry = pair_call([(0, 0, 0)] * PIECES, own, 0, PIECES, band, positions, row_shift, row_charge, None, site_block)
        carry = carry[:2] + (jnp.zeros((1,), jnp.int32),)

        carry, a, twin = gate((carry, a, twin))
        for t in twin:
            arrive(t, 1)
        arrive(a, 0)
        flip_a = swap(a, near)
        carry = sum_some(carry, QUOTAS[0])

        carry, a, b, flip_a = gate((carry, a, b, flip_a))
        two_a, two_b, flip_b = hop(a, second), hop(b, second), swap(b, near)
        arrive(flip_a, 1)
        arrive(b, 0)
        carry = sum_some(carry, QUOTAS[1])

        carry, a, b, two_a, two_b, flip_b = gate((carry, a, b, two_a, two_b, flip_b))
        a, b = {**a, **two_a}, {**b, **two_b}
        three_a, three_b, flip_2a, flip_2b = hop(a, third), hop(b, third), swap(two_a, second), swap(two_b, second)
        arrive(flip_b, 1)
        arrive(two_a, 0)
        arrive(two_b, 0)
        carry = sum_some(carry, QUOTAS[2])

        carry, a, b, three_a, three_b, flip_2a, flip_2b = gate((carry, a, b, three_a, three_b, flip_2a, flip_2b))
        a, b = {**a, **three_a}, {**b, **three_b}
        four_a, four_b, flip_3a, flip_3b = last_hop(a, 0), last_hop(b, 1), swap(three_a, third), swap(three_b, third)
        for held, flip in ((flip_2a, 1), (flip_2b, 1), (three_a, 0), (three_b, 0)):
            arrive(held, flip)
        carry = sum_some(carry, QUOTAS[3])

        carry, four_a, four_b, flip_3a, flip_3b = gate((carry, four_a, four_b, flip_3a, flip_3b))
        flip_4a, flip_4b = swap(four_a, four_a), swap(four_b, four_b)
        for held, flip in ((flip_3a, 1), (flip_3b, 1), (four_a, 0), (four_b, 0)):
            arrive(held, flip)
        carry = sum_some(carry, QUOTAS[4])

        carry, flip_4a, flip_4b = gate((carry, flip_4a, flip_4b))
        arrive(flip_4a, 1)
        arrive(flip_4b, 1)
        forces, share, _ = sum_some(carry, len(queue), True)
        energy = 0.5 * jnp.sum(energy_call(share, seg_len))
        return forces, energy.reshape(1)

    row_spec = P(('sys', 'seg'), None)
    vec_spec = P(('sys', 'seg'))
    return jax.shard_map(device_fn, mesh=mesh, in_specs=(row_spec, vec_spec, row_spec), out_specs=(row_spec, P('sys')), check_vma=False)
```

```python
import functools
import math

import jax
import jax.numpy as jnp
from jax import lax
from jax.experimental import pallas as pl
from jax.experimental.pallas import tpu as pltpu
from jax.sharding import PartitionSpec as P


TILE_ROWS = 512
TILE_COLS = 1024
PIECES = 2
VMEM_LIMIT = 67043328
QUOTAS = (4, 8, 8, 9)
AUX_ROWS = 16
EDGE = 99
LOG2E = math.log2(math.e)


def split3(v):
    hi = v.astype(jnp.bfloat16).astype(jnp.float32)
    rest = v - hi
    mid = rest.astype(jnp.bfloat16).astype(jnp.float32)
    return hi, mid, rest - mid


def pack_call(x_rows, charges):
    n_rows, feat = x_rows.shape
    piece = n_rows // PIECES
    step = 128

    def kernel(x_ref, q_ref, *refs):
        packs, (shift_ref, charge_ref, flat) = refs[:PIECES], refs[PIECES:]

        @pl.loop(0, n_rows // step)
        def _(b):
            rows = pl.ds(pl.multiple_of(b * step, step), step)
            x32 = x_ref[rows, :].astype(jnp.float32)
            shift = jnp.sum(x32 * x32, axis=1, keepdims=True) * (-0.5 / feat * LOG2E)
            shift = jnp.broadcast_to(shift, (step, step))
            shift_ref[rows, :] = shift
            q_row = q_ref[pl.ds(b, 1), :]
            charge_ref[rows, :] = jnp.broadcast_to(q_row, (step, step)).T
            flat[0, :, rows] = shift.T[:1, :]
            flat[1, :, rows] = q_row

        for h in range(PIECES):
            @pl.loop(0, piece // step)
            def _(b, h=h):
                rows = pl.ds(pl.multiple_of(b * step, step), step)
                packs[h][rows, :] = x_ref[pl.ds(pl.multiple_of(h * piece + b * step, step), step), :]

            aux = []
            for v in range(2):
                for part in split3(flat[v, :, h * piece:(h + 1) * piece]):
                    aux.append(part[:, :feat])
                    aux.append(jnp.concatenate([part[:, feat:], jnp.zeros((1, 2 * feat - piece), jnp.float32)], axis=1))
            aux.append(jnp.zeros((AUX_ROWS - len(aux), feat), jnp.float32))
            packs[h][piece:, :] = jnp.concatenate(aux, axis=0).astype(jnp.bfloat16)

    vmem = pl.BlockSpec(memory_space=pltpu.VMEM)
    spread = jax.ShapeDtypeStruct((n_rows, step), jnp.float32)
    return pl.pallas_call(
        kernel,
        out_shape=[jax.ShapeDtypeStruct((piece + AUX_ROWS, feat), jnp.bfloat16)] * PIECES + [spread, spread],
        in_specs=[vmem, vmem],
        out_specs=[vmem] * (PIECES + 2),
        scratch_shapes=[pltpu.VMEM((2, 1, n_rows), jnp.float32)],
        name="pack_rows",
    )(x_rows, charges.reshape(n_rows // step, step))


def pair_call(sites, cols, done, quota, band, x_rows, row_shift, row_charge, carry, site_block, final=False):
    n_rows, feat = x_rows.shape
    piece = cols[0].shape[0] - AUX_ROWS
    n_bufs = len(cols)
    inv_lsq = 1.0 / feat
    dot_scale = inv_lsq * LOG2E
    tr, tc = TILE_ROWS, TILE_COLS
    n_chunk = piece // tc
    n_bands = n_rows // tr
    n_tiles = n_bands * n_chunk
    first = carry is None

    def kernel(*refs):
        band_ref, shift_in, charge_in, x_hbm = refs[:4]
        refs = refs[4:]
        col_refs, refs = refs[:n_bufs], refs[n_bufs:]
        if not first:
            (p_in, r_in, next_in), refs = refs[:3], refs[3:]
        (p_out, r_out, next_out), refs = refs[:3], refs[3:]
        x_v, p_v, r_v, shift_v, charge_v, col_v, aux_v, dot_v, list_ref, sems, x_sems, row_sems, share_sem = refs

        n_live = jnp.int32(0)
        start = jnp.int32(0) if first else next_in[0]
        nxt = start
        for k, site in enumerate(sites):
            col, ok = site_block(site)
            take = ok & (band_ref[0, col] != 0) & (start <= done + k) & (n_live < quota)
            list_ref[n_live] = k
            n_live = n_live + take.astype(jnp.int32)
            nxt = jnp.where((start <= done + k) & ((n_live < quota) | take), done + k + 1, nxt)
        next_out[0] = nxt
        n_all = n_live * n_tiles

        def col_start(item):
            slot = list_ref[item]
            par = lax.rem(item, 2)
            for k in range(n_bufs):
                @pl.when(slot == k)
                def _(k=k):
                    pltpu.make_async_copy(col_refs[k], col_v.at[par], sems.at[par]).start()

        def col_wait(item):
            par = lax.rem(item, 2)
            pltpu.make_async_copy(col_refs[0], col_v.at[par], sems.at[par]).wait()
            aux = col_v[par, piece:, :].astype(jnp.float32)
            for v in range(2):
                r = 6 * v
                wide = aux[r:r + 1, :] + aux[r + 2:r + 3, :] + aux[r + 4:r + 5, :]
                tail = aux[r + 1:r + 2, :] + aux[r + 3:r + 4, :] + aux[r + 5:r + 6, :]
                aux_v[par, v, :, :feat] = wide
                aux_v[par, v, :, feat:] = tail[:, :piece - feat]

        def place(t):
            item = t // n_tiles
            local = lax.rem(t, n_tiles)
            row0 = pl.multiple_of((local // n_chunk) * tr, tr)
            col0 = pl.multiple_of(lax.rem(local, n_chunk) * tc, tc)
            return item, row0, col0

        def dots(t, dst):
            item, row0, col0 = place(jnp.minimum(t, n_all - 1))
            dot_v[dst] = lax.dot_general(
                x_v[pl.ds(row0, tr), :], col_v[lax.rem(item, 2), pl.ds(col0, tc), :],
                (((1,), (1,)), ((), ())), preferred_element_type=jnp.float32)

        def pulls(t, src):
            item, row0, col0 = place(t)
            par = lax.rem(item, 2)
            shift_r = shift_v[pl.ds(row0, tr), :]
            charge_r = charge_v[pl.ds(row0, tr), :]
            if first:
                gap = lax.broadcasted_iota(jnp.int32, (tr, 128), 1) - lax.broadcasted_iota(jnp.int32, (tr, 128), 0)
                diag = row0 - list_ref[item] * piece - col0
            row_sum = None
            low = []
            for j in range(tc // 128):
                at = pl.multiple_of(col0 + j * 128, 128)
                shift_c = aux_v[par, 0, :, pl.ds(at, 128)]
                charge_c = aux_v[par, 1, :, pl.ds(at, 128)]
                expo = jnp.minimum(dot_v[src, :, j * 128:(j + 1) * 128] * dot_scale + (shift_r + shift_c), 0.0)
                w = jnp.exp2(expo) * (charge_r * charge_c)
                if first:
                    w = jnp.where(gap + j * 128 == diag, 0.0, w)
                row_sum = w if row_sum is None else row_sum + w
                low.append(w.astype(jnp.bfloat16))
            r_v[pl.ds(row0, tr), :] += row_sum
            p_v[pl.ds(row0, tr), :] += jnp.dot(
                jnp.concatenate(low, axis=1), col_v[par, pl.ds(col0, tc), :], preferred_element_type=jnp.float32)

        def rows_of(i):
            return pl.ds(pl.multiple_of(i * tr, tr), tr)

        def x_load(i):
            return pltpu.make_async_copy(x_hbm.at[rows_of(i)], x_v.at[rows_of(i)], x_sems.at[i])

        def row_loads(i):
            pairs = [(shift_in, shift_v), (charge_in, charge_v)]
            if not first:
                pairs += [(p_in, p_v), (r_in, r_v)]
            return [pltpu.make_async_copy(src.at[rows_of(i)], dst.at[rows_of(i)], row_sems.at[k, i])
                    for k, (src, dst) in enumerate(pairs)]

        def p_store(i):
            return pltpu.make_async_copy(p_v.at[rows_of(i)], p_out.at[rows_of(i)], row_sems.at[2, i])

        def row_stores(i):
            return [p_store(i), pltpu.make_async_copy(r_v.at[rows_of(i)], r_out.at[rows_of(i)], row_sems.at[3, i])]

        def load_pair(j):
            for i in (j + 1, j + 2):
                if i < n_bands:
                    x_load(i).start()
            for i in (j, j + 1):
                for c in row_loads(i):
                    c.start()

        def wait_pair(j):
            for i in (j + 1, j + 2):
                if i < n_bands:
                    x_load(i).wait()
            for i in (j, j + 1):
                for c in row_loads(i):
                    c.wait()

        def sums():
            col_start(0)
            x_load(0).start()
            if first:
                @pl.loop(0, n_rows // 128)
                def _(i):
                    rows = pl.ds(pl.multiple_of(i * 128, 128), 128)
                    p_v[rows, :] = jnp.zeros((128, feat), jnp.float32)
                    r_v[rows, :] = jnp.zeros((128, 128), jnp.float32)

            col_wait(0)
            x_load(0).wait()
            load_pair(0)
            dots(0, 0)

            @pl.loop(0, n_all // 2)
            def _(u):
                t = u * 2
                item = t // n_tiles
                local = lax.rem(t, n_tiles)

                @pl.when((local == 0) & (item + 1 < n_live))
                def _():
                    col_start(item + 1)

                for j in range(0, n_bands, 2):
                    @pl.when(t == j)
                    def _(j=j):
                        wait_pair(j)
                        if j + 2 < n_bands:
                            load_pair(j + 2)

                @pl.when((local + 2 == n_tiles) & (item + 1 < n_live))
                def _():
                    col_wait(item + 1)

                dots(t + 1, 1)
                pulls(t, 0)
                dots(t + 2, 0)
                pulls(t + 1, 1)

                if not final:
                    @pl.when(item + 1 == n_live)
                    def _():
                        for c in row_stores(local) + row_stores(local + 1):
                            c.start()

            if not final:
                for i in range(n_bands):
                    for c in row_stores(i):
                        c.wait()

        @pl.when(n_live > 0)
        def _():
            sums()

        if final:
            @pl.when(n_live == 0)
            def _():
                x_load(0).start()
                for j in range(0, n_bands, 2):
                    load_pair(j)
                x_load(0).wait()
                for j in range(0, n_bands, 2):
                    wait_pair(j)

            @pl.loop(0, n_rows // 128, init_carry=jnp.zeros((8, 128), jnp.float32))
            def share(i, so_far):
                rows = pl.ds(pl.multiple_of(i * 128, 128), 128)
                lanes = r_v[rows, :]
                total = jnp.sum(lanes, axis=1, keepdims=True)
                p_v[rows, :] = (total * x_v[rows, :].astype(jnp.float32) - p_v[rows, :]) * inv_lsq

                @pl.when((i + 1) % (tr // 128) == 0)
                def _():
                    p_store(i // (tr // 128)).start()

                for g in range(16):
                    so_far = so_far + lanes[g * 8:(g + 1) * 8, :]
                return so_far

            r_v[:8, :] = share
            share_out = pltpu.make_async_copy(r_v.at[:8], r_out, share_sem)
            share_out.start()
            for i in range(n_bands):
                p_store(i).wait()
            share_out.wait()

    assert n_chunk == 1 and n_tiles % 2 == 0
    smem = pl.BlockSpec(memory_space=pltpu.SMEM)
    hbm = pl.BlockSpec(memory_space=pl.ANY)
    args = [band, row_shift, row_charge, x_rows] + list(cols)
    specs = [smem, hbm, hbm, hbm] + [hbm] * n_bufs
    aliases = {}
    if not first:
        aliases = {len(args): 0} if final else {len(args): 0, len(args) + 1: 1}
        args += list(carry)
        specs += [hbm, hbm, smem]
    flops = int(4 * n_rows * piece * feat * min(quota, 2 * n_bufs // 3 + 1))
    return pl.pallas_call(
        kernel,
        out_shape=(jax.ShapeDtypeStruct((n_rows, feat), jnp.float32),
                   jax.ShapeDtypeStruct((8 if final else n_rows, 128), jnp.float32),
                   jax.ShapeDtypeStruct((1,), jnp.int32)),
        in_specs=specs,
        out_specs=(hbm, hbm, smem),
        input_output_aliases=aliases,
        scratch_shapes=[
            pltpu.VMEM((n_rows, feat), jnp.bfloat16),
            pltpu.VMEM((n_rows, feat), jnp.float32),
            pltpu.VMEM((n_rows, 128), jnp.float32),
            pltpu.VMEM((n_rows, 128), jnp.float32),
            pltpu.VMEM((n_rows, 128), jnp.float32),
            pltpu.VMEM((2, piece + AUX_ROWS, feat), jnp.bfloat16),
            pltpu.VMEM((2, 2, 1, piece), jnp.float32),
            pltpu.VMEM((2, tr, tc), jnp.float32),
            pltpu.SMEM((n_bufs + 1,), jnp.int32),
            pltpu.SemaphoreType.DMA((2,)),
            pltpu.SemaphoreType.DMA((n_bands,)),
            pltpu.SemaphoreType.DMA((4, n_bands)),
            pltpu.SemaphoreType.DMA,
        ],
        cost_estimate=pl.CostEstimate(flops=flops, bytes_accessed=4 * n_rows * feat * 4, transcendentals=0),
        compiler_params=pltpu.CompilerParams(vmem_limit_bytes=VMEM_LIMIT),
        name="pair_pulls",
    )(*args)


def energy_call(part, seg_len):
    def kernel(part_ref, out_ref, held, send_sems, recv_sems):
        me = lax.axis_index('seg')
        barrier = pltpu.get_barrier_semaphore()
        for k in range(1, seg_len):
            pl.semaphore_signal(barrier, inc=1, device_id={'seg': lax.rem(me + k, seg_len)})
        pl.semaphore_wait(barrier, seg_len - 1)
        copies = [pltpu.make_async_remote_copy(
            src_ref=part_ref, dst_ref=held.at[me], send_sem=send_sems.at[k], recv_sem=recv_sems.at[k],
            device_id={'seg': lax.rem(me + k, seg_len)}) for k in range(1, seg_len)]
        for c in copies:
            c.start()
        held[me] = part_ref[...]
        for c in copies:
            c.wait()
        total = held[0]
        for k in range(1, seg_len):
            total = total + held[k]
        out_ref[...] = total

    vmem = pl.BlockSpec(memory_space=pltpu.VMEM)
    return pl.pallas_call(
        kernel,
        out_shape=jax.ShapeDtypeStruct(part.shape, jnp.float32),
        in_specs=[vmem],
        out_specs=vmem,
        scratch_shapes=[pltpu.VMEM((seg_len,) + part.shape, jnp.float32),
                        pltpu.SemaphoreType.DMA((seg_len,)), pltpu.SemaphoreType.DMA((seg_len,))],
        compiler_params=pltpu.CompilerParams(collective_id=0, has_side_effects=True),
        name="energy_sum",
    )(part)


def solution(mesh):
    seg_len = mesh.shape['seg']
    side = math.isqrt(seg_len // 2)
    assert 2 * side * side == seg_len and side & (side - 1) == 0

    def dev(x, y, core):
        return ((y % side) * side + x % side) * 2 + core

    grid = [(x, y, core) for y in range(side) for x in range(side) for core in range(2)]

    def come_from(values, dx, dy):
        return lax.ppermute(values, 'seg', [(dev(x + dx, y + dy, c), dev(x, y, c)) for x, y, c in grid])

    def other_core(value):
        return lax.ppermute(value, 'seg', [(dev(x, y, 1 - c), dev(x, y, c)) for x, y, c in grid])

    def device_fn(positions, charges, pair_band):
        reach = (pair_band.shape[1] - 1) // 2

        def site_block(site):
            dx, dy, flip = site
            me = lax.axis_index('seg')
            core, chip = me & 1, me >> 1
            x, y = chip & (side - 1), chip >> (side.bit_length() - 1)
            if dx == EDGE:
                dx = jnp.where(x == 0, side - 1, jnp.where(x == side - 1, 1, 0))
            else:
                dx = dx % side
            blk = (((y + dy % side) & (side - 1)) * side + ((x + dx) & (side - 1))) * 2 + ((core + flip) & 1)
            gap = ((blk - me + seg_len + seg_len // 2) & (seg_len - 1)) - seg_len // 2
            ok = (gap <= reach) & (gap >= -reach)
            if site[0] == EDGE:
                ok = ok & ((x == 0) | (x == side - 1))
            return jnp.where(ok, gap + reach, 0), ok

        pack_and_rows = pack_call(positions, charges)
        own, (row_shift, row_charge) = pack_and_rows[:PIECES], pack_and_rows[PIECES:]
        band = pair_band
        axis_y = lax.axis_index('seg') // 2
        my_x = lax.rem(axis_y, side)

        near = ((1, 0), (-1, 0), (0, 1), (0, -1))
        second = {(2, 0): ((1, 0), (1, 0)), (-1, -1): ((0, -1), (-1, 0)), (1, 1): ((1, 0), (0, 1)), (1, -1): ((1, 0), (0, -1))}
        third = {(-1, 1): ((0, 1), (-1, 0)), (2, 1): ((2, 0), (0, 1)), (2, -1): ((2, 0), (0, -1))}
        edge_perm = [(dev(0, y + 1, c), dev(0, y, c)) for y in range(side) for c in range(2)]
        edge_perm += [(dev(side - 1, y - 1, c), dev(side - 1, y, c)) for y in range(side) for c in range(2)]

        def hop(held, table):
            return {off: come_from(held[src], *step) for off, (src, step) in table.items()}

        def cross_perm(column, most, few):
            return [(dev(x, y + (few if x == column else most), c), dev(x, y, c)) for x, y, c in grid]

        def last_hop(held, h):
            column, most, few = ((0, 1, -1), (side - 1, -1, 1))[h % 2]
            cross = jnp.where(my_x == column, held[(2, few)], held[(2, most)])
            edge = jnp.where(my_x == 0, held[(-1, 1)], held[(1, -1)])
            return {(2, 2): lax.ppermute(cross, 'seg', cross_perm(column, most, few)),
                    (EDGE, 2): lax.ppermute(edge, 'seg', edge_perm)}

        def swap(held, offs):
            return {off: other_core(held[off]) for off in offs}

        queue = []
        lowest = [0]

        def arrive(held, flip):
            for off, value in held.items():
                queue.append((off + (flip,), value))

        def sum_some(carry, quota, final=False):
            low = lowest[0]
            sites, cols = zip(*queue[low:])
            lowest[0] = min(len(queue), low + quota)
            return pair_call(sites, cols, low, quota, band, positions, row_shift, row_charge, carry, site_block, final)

        gate = lax.optimization_barrier
        twin = [{(0, 0): other_core(o)} for o in own]
        a, b = [{off: come_from(o, *off) for off in near} for o in own]
        carry = pair_call([(0, 0, 0)] * PIECES, own, 0, PIECES, band, positions, row_shift, row_charge, None, site_block)
        carry = carry[:2] + (jnp.zeros((1,), jnp.int32),)

        carry, a, twin = gate((carry, a, twin))
        for t in twin:
            arrive(t, 1)
        arrive(a, 0)
        flip_a = swap(a, near)
        carry = sum_some(carry, QUOTAS[0])

        carry, a, b, flip_a = gate((carry, a, b, flip_a))
        two_a, two_b, flip_b = hop(a, second), hop(b, second), swap(b, near)
        arrive(flip_a, 1)
        arrive(b, 0)
        carry = sum_some(carry, QUOTAS[1])

        carry, a, b, two_a, two_b, flip_b = gate((carry, a, b, two_a, two_b, flip_b))
        a, b = {**a, **two_a}, {**b, **two_b}
        three_a, three_b, flip_2a, flip_2b = hop(a, third), hop(b, third), swap(two_a, second), swap(two_b, second)
        arrive(flip_b, 1)
        arrive(two_a, 0)
        arrive(two_b, 0)
        carry = sum_some(carry, QUOTAS[2])

        carry, a, b, three_a, three_b, flip_2a, flip_2b = gate((carry, a, b, three_a, three_b, flip_2a, flip_2b))
        a, b = {**a, **three_a}, {**b, **three_b}
        four_a, four_b, flip_3a, flip_3b = last_hop(a, 0), last_hop(b, 1), swap(three_a, third), swap(three_b, third)
        for held, flip in ((flip_2a, 1), (flip_2b, 1), (three_a, 0), (three_b, 0)):
            arrive(held, flip)
        carry = sum_some(carry, QUOTAS[3])

        carry, four_a, four_b, flip_3a, flip_3b = gate((carry, four_a, four_b, flip_3a, flip_3b))
        flip_4a, flip_4b = swap(four_a, four_a), swap(four_b, four_b)
        for held, flip in ((flip_3a, 1), (flip_3b, 1), (four_a, 0), (four_b, 0)):
            arrive(held, flip)

        flip_4a, flip_4b = gate((flip_4a, flip_4b))
        arrive(flip_4a, 1)
        arrive(flip_4b, 1)
        forces, share, _ = sum_some(carry, len(queue), True)
        energy = 0.5 * jnp.sum(energy_call(share, seg_len))
        return forces, energy.reshape(1)

    row_spec = P(('sys', 'seg'), None)
    vec_spec = P(('sys', 'seg'))
    return jax.shard_map(device_fn, mesh=mesh, in_specs=(row_spec, vec_spec, row_spec), out_specs=(row_spec, P('sys')), check_vma=False)
```
